32 devices in a mesh: gx: 8 (over y, x, core), gy: 4 (over z).
Axes of the slice: x: 2, y: 2, z: 4, core: 2. Of those that a mesh axis runs over, the one named last changes fastest.
Arguments:
- core_one: bfloat16 [200, 128], replicated, may hold values from -6 to 6
- core_two: bfloat16 [200, 4096], replicated, may hold values from -1 to 1
- core_three: bfloat16 [250, 256], replicated, may hold values from -1 to 1
- dense_rows: bfloat16 [2048, 128], P(('gx', 'gy')), may hold values from -6 to 6
- w_top: bfloat16 [256, 256], replicated, may hold values from -0.375 to 0.375
- bias_top: float32 [256], replicated, may hold values from -3 to 3
- w_out: float32 [256], replicated, may hold values from -0.75 to 0.75
- labels: int32 [2048], P(('gx', 'gy')), may hold values 0 or 1
- bag_ids: int32 [32, 256], P(('gx', 'gy')), may hold values from 0 to 63, never falling along the last dimension, each value on 1 to 8 neighbouring positions
- digit_one: int32 [32, 256], P(('gx', 'gy')), may hold values from 0 to 199
- digit_two: int32 [32, 256], P(('gx', 'gy')), may hold values from 0 to 199
- digit_three: int32 [32, 256], P(('gx', 'gy')), may hold values from 0 to 249
Outputs:
- core_grad: float32 [908800], P(('gx', 'gy'))
- top_grad: float32 [258, 256], replicated
The draws below stay inside these ranges and needn't reach their ends.
Inputs may be any that keep to these rules, and one draw needn't show every extreme that they name: `bag_ids`: along a row, never falling; every sample of the block gets 1 to 8 lookups, one exactly 8.
All inputs are finite; a program needn't handle non-finite values. No bound on the sum of `labels` on one device may be relied on, other than what follows from the above.
Results may differ from the reference program's by a relative error of at most 0.0018.
The reference program's roundings to bfloat16 on the way (of `joined` and `dpre`) count: a program that leaves them out, or rounds other values in their place, can miss the bound.
Values sent between devices are 32-bit elements; how exact they have to be, the bound alone decides.
No kernel may reach another device: no remote copies, remote signals or barrier semaphores. Data moves between devices by JAX's collectives and lax.ppermute only.
A program may use at most 64 MiB of HBM per device.

```python
import math
import jax
import jax.numpy as jnp
import numpy as np
from jax import lax

N1 = 200
N2 = 200
N3 = 250
D1 = 4
D2 = 4
D3 = 8
R = 32
HID = 256
BAG_MOST = 8
BATCH_DEV = 64
DIM = 128
LOOKS = 256
BATCH = 2048
N_GX = 8
N_GY = 4
DEVICES = 32


def touch_ends(drawn, rng, low, largest):
    longest = drawn.shape.index(max(drawn.shape))
    spots = []
    for shift in (0, 1):
        where = [jax.random.randint(jax.random.fold_in(rng, axis), (), 0, length) for axis, length in enumerate(drawn.shape)]
        where[longest] = (where[longest] + shift) % drawn.shape[longest]
        spots.append(tuple(where))
    return drawn.at[spots[0]].set(low).at[spots[1]].set(largest)


def spiked(array, stream_key, source, target, blocks, factor):
    owner, partner = [(jnp.arange(array.shape[position]) // (array.shape[position] // blocks)).reshape([-1 if axis == position else 1 for axis in range(array.ndim)]) for position in (source, target)]
    chosen = jax.random.permutation(stream_key, blocks)[partner]
    strong = (owner == chosen) | (owner == (partner + blocks // 2) % blocks)
    return jnp.where(strong, factor * array, array)


def levels(stream_key, dims, cuts, smallest, top_value):
    def one(dim, shards_of):
        steps = jax.random.uniform(jax.random.fold_in(jax.random.fold_in(stream_key, 6), dim), (shards_of,), jnp.float32, smallest / len(cuts), top_value / len(cuts))
        return jnp.repeat(jnp.exp(steps), dims[dim] // shards_of).reshape((-1,) + (1,) * (len(dims) - dim - 1))

    factor_of = one(*cuts[0])
    for cut in cuts[1:]:
        factor_of = factor_of * one(*cut)
    return factor_of


def split_up(amount, total, reach, slope):
    loads = [(1 << 20) // math.isqrt(standing ** slope) + 1 for standing in range(2, amount + 1)]
    spare, given = total - reach - (amount - 1), [1] * (amount - 1)
    while spare > 0:
        movable = [i for i in range(amount - 1) if given[i] < reach]
        pool, left = sum([loads[i] for i in movable]), spare
        for i in movable:
            more = min(reach - given[i], max(1, left * loads[i] // pool), spare)
            given[i] = given[i] + more
            spare = spare - more
    return np.array([reach] + given)


def uneven_parts(key, number_of, total, reach, slope):
    if number_of == 2:
        one = jax.random.randint(key, (), max(1, total - reach), min(reach, total - 1) + 1)
        return jnp.stack([one, total - one])
    sizes = jnp.asarray(split_up(number_of, total, reach, slope), jnp.int32)
    pairs = (number_of - 1) // 2
    giver, receiver = sizes[1:1 + 2 * pairs:2], sizes[2:2 + 2 * pairs:2]
    room = jnp.minimum(giver - 1, reach - receiver)
    passed = jax.random.randint(jax.random.fold_in(key, 1), (pairs,), 0, 1 << 20) % (room + 1)
    sizes = sizes.at[1:1 + 2 * pairs:2].set(giver - passed).at[2:2 + 2 * pairs:2].set(receiver + passed)
    return sizes[jax.random.permutation(jax.random.fold_in(key, 2), number_of)]


def bell_draw(stream_key, shape, spread, most, cuts=(), kind=jnp.bfloat16):
    level = levels(stream_key, shape, cuts, -0.22, 0.18) if cuts else 1.0
    array = jax.random.normal(stream_key, shape, jnp.float32) * spread * level
    return jnp.minimum(jnp.maximum(array, -most), most).astype(kind)


def heavy_noise(key, shape, width, limit, cuts, heavy, held_as=jnp.bfloat16):
    result = width * jax.random.normal(key, shape, jnp.float32)
    if cuts:
        result = result * levels(key, shape, cuts, -0.22, 0.18)
    return jnp.clip(spiked(result, jax.random.fold_in(key, 3), *heavy), -limit, limit).astype(held_as)


def setup_inputs(seed: int = 0) -> dict:
    keys = jax.random.split(jax.random.key(seed), 13)
    core_one = bell_draw(keys[0], (N1, D1 * R), 1.0, 6.0)
    core_two = bell_draw(keys[1], (N2, R * D2 * R), R ** -0.5, 1.0)
    core_three = bell_draw(keys[2], (N3, R * D3), R ** -0.5, 1.0)
    dense_rows = heavy_noise(keys[3], (BATCH, DIM), 1.0, 6.0, ((0, 32),), (0, 1, 32, 2.75))
    w_top = bell_draw(keys[4], (2 * DIM, HID), (2 * DIM) ** -0.5, 0.375)
    bias_top = bell_draw(keys[5], (HID,), 0.5, 3.0, (), jnp.float32)
    w_out = bell_draw(keys[6], (HID,), (HID // 4) ** -0.5, 0.75, (), jnp.float32)
    labels = touch_ends((jax.random.randint(keys[7], (BATCH,), 0, 4) < 1).astype(jnp.int32), jax.random.fold_in(keys[7], 1), 0, 1)
    bag_ids = jax.vmap(lambda own: jnp.searchsorted(jnp.cumsum(uneven_parts(own, BATCH_DEV, LOOKS, BAG_MOST, 1)), jnp.arange(LOOKS), side="right"))(jax.random.split(keys[8], DEVICES)).reshape((DEVICES, LOOKS)).astype(jnp.int32)
    digit_one = touch_ends(jax.random.randint(keys[9], (DEVICES, LOOKS), 0, N1), jax.random.fold_in(keys[9], 1), 0, N1 - 1).astype(jnp.int32)
    digit_two = touch_ends(jax.random.randint(keys[10], (DEVICES, LOOKS), 0, N2), jax.random.fold_in(keys[10], 1), 0, N2 - 1).astype(jnp.int32)
    digit_three = touch_ends(jax.random.randint(keys[11], (DEVICES, LOOKS), 0, N3), jax.random.fold_in(keys[11], 1), 0, N3 - 1).astype(jnp.int32)
    return {"core_one": core_one, "core_two": core_two, "core_three": core_three, "dense_rows": dense_rows, "w_top": w_top, "bias_top": bias_top, "w_out": w_out, "labels": labels, "bag_ids": bag_ids, "digit_one": digit_one, "digit_two": digit_two, "digit_three": digit_three}


def reference(core_one, core_two, core_three, dense_rows, w_top, bias_top, w_out, labels, bag_ids, digit_one, digit_two, digit_three):
    high = lax.Precision.HIGHEST
    groups = N_GX * N_GY
    dense_view = dense_rows.reshape(groups, BATCH_DEV, DIM)
    label_view = labels.reshape(groups, BATCH_DEV)

    def device_terms(carry, item):
        dense_block, label_block, bags, first_digit, second_digit, third_digit = item
        first = core_one[first_digit].astype(jnp.float32).reshape(-1, D1, R)
        middle = core_two[second_digit].astype(jnp.float32).reshape(-1, R, D2 * R)
        last = core_three[third_digit].astype(jnp.float32).reshape(-1, R, D3)
        left = jnp.einsum("nia,nab->nib", first, middle, precision=high).reshape(-1, D1 * D2, R)
        embedded = jnp.einsum("npa,nad->npd", left, last, precision=high).reshape(-1, D1 * D2 * D3)
        pooled = jax.ops.segment_sum(embedded, bags, num_segments=BATCH_DEV)
        joined = jnp.concatenate([dense_block, pooled.astype(jnp.bfloat16)], axis=1)
        pre = jnp.dot(joined, w_top, preferred_element_type=jnp.float32) + bias_top[None, :]
        sig = jax.nn.sigmoid(pre)
        hidden = pre * sig
        logit = jnp.dot(hidden, w_out, precision=high)
        dlogit = (jax.nn.sigmoid(logit) - label_block.astype(jnp.float32)) / BATCH_DEV
        dpre = dlogit[:, None] * w_out[None, :] * (sig * (1.0 + pre * (1.0 - sig)))
        dpre_low = dpre.astype(jnp.bfloat16)
        grad_weight = jnp.dot(joined.T, dpre_low, preferred_element_type=jnp.float32)
        grad_bias = jnp.sum(dpre, axis=0)
        grad_output = jnp.sum(hidden * dlogit[:, None], axis=0)
        top_local = jnp.concatenate([grad_weight, grad_bias[None, :], grad_output[None, :]], axis=0)
        grad_pooled = jnp.dot(dpre_low, w_top[D1 * D2 * D3:].T, preferred_element_type=jnp.float32)
        grad_view = grad_pooled[bags].reshape(-1, D1 * D2, D3)
        grad_last = jnp.einsum("npa,npd->nad", left, grad_view, precision=high)
        grad_left = jnp.einsum("npd,nad->npa", grad_view, last, precision=high).reshape(-1, D1, D2 * R)
        grad_first = jnp.einsum("nib,nab->nia", grad_left, middle, precision=high)
        grad_middle = jnp.einsum("nia,nib->nab", first, grad_left, precision=high)
        sum_first = jax.ops.segment_sum(grad_first.reshape(-1, D1 * R), first_digit, num_segments=N1)
        sum_middle = jax.ops.segment_sum(grad_middle.reshape(-1, R * D2 * R), second_digit, num_segments=N2)
        sum_last = jax.ops.segment_sum(grad_last.reshape(-1, R * D3), third_digit, num_segments=N3)
        return (carry[0] + sum_first, carry[1] + sum_middle, carry[2] + sum_last, carry[3] + top_local), None

    start = (jnp.zeros((N1, D1 * R), jnp.float32), jnp.zeros((N2, R * D2 * R), jnp.float32),
             jnp.zeros((N3, R * D3), jnp.float32), jnp.zeros((2 * D1 * D2 * D3 + 2, HID), jnp.float32))
    totals, _ = lax.scan(device_terms, start, (dense_view, label_view, bag_ids, digit_one, digit_two, digit_three))
    core_grad = jnp.concatenate([totals[0].reshape(-1), totals[1].reshape(-1), totals[2].reshape(-1)])
    return core_grad, totals[3]
```

```python
import functools

import jax
import jax.numpy as jnp
from jax import lax
from jax.experimental import pallas as pl
from jax.experimental.pallas import tpu as pltpu
from jax.sharding import PartitionSpec as P


D1 = 4
D2 = 4
D3 = 8
R = 32
LANES = 128
F32 = jnp.float32
BF16 = jnp.bfloat16
TN = (((0,), (0,)), ((), ()))
NT = (((1,), (1,)), ((), ()))
VMEM_LIMIT = 60 * 1024 * 1024


def up(value, step):
    return -(-value // step) * step


def dot(a, b, dims):
    return lax.dot_general(a, b, dims, preferred_element_type=F32)


def nn(a, b):
    return jnp.dot(a, b, preferred_element_type=F32)


def split(x, count=2):
    terms = []
    for _ in range(count):
        terms.append(x.astype(BF16))
        x = x - terms[-1].astype(F32)
    return terms


def one_hot_rows(row, count):
    grid = lax.broadcasted_iota(jnp.int32, (count, row.shape[1]), 0)
    return jnp.where(grid == row, 1.0, 0.0).astype(BF16)


def sections(n1, n3, hid, top_rows):
    halves = hid // LANES
    top = [part * up(top_rows, 8) for part in range(halves)]
    ones = halves * up(top_rows, 8)
    wide = (R * D3) // LANES
    lasts = [ones + up(n1, 8) + part * up(n3, 8) for part in range(wide)]
    return top, ones, lasts, lasts[-1] + up(n3, 8)


def expand_left(first, middle, left, looks):
    def block(step, _):
        lanes = pl.ds(pl.multiple_of((step // 4) * LANES, LANES), LANES)
        base = (step % 4) * R
        totals = [jnp.zeros((R, LANES), F32) for _ in range(D1)]
        for a in range(R):
            rows = middle[pl.ds(a * D2 * R + base, R), lanes]
            for i in range(D1):
                totals[i] += first[i * R + a : i * R + a + 1, lanes] * rows
        for i in range(D1):
            left[pl.ds(i * D2 * R + base, R), lanes] = totals[i]
        return 0

    lax.fori_loop(0, (looks // LANES) * D2, block, 0)


def lanes_of(half):
    return pl.ds(pl.multiple_of(half * LANES, LANES), LANES)


def expand_embedded(left, last, out, looks):
    def one(half, _):
        lanes = lanes_of(half)
        totals = [jnp.zeros((D3, LANES), F32) for _ in range(D1 * D2)]
        for b in range(R):
            rows = last[half, b * D3 : (b + 1) * D3, :]
            for p in range(D1 * D2):
                totals[p] += left[p * R + b : p * R + b + 1, lanes] * rows
        for p in range(D1 * D2):
            out[p * D3 : (p + 1) * D3, lanes] = totals[p]
        return 0

    lax.fori_loop(0, looks // LANES, one, 0)


def expand_grad_left(grad, last, out, lanes):
    turned = [last[pl.ds(d, R, stride=D3), :] for d in range(D3)]
    for p in range(D1 * D2):
        total = jnp.zeros((R, LANES), F32)
        for d in range(D3):
            total += grad[p * D3 + d : p * D3 + d + 1, lanes] * turned[d]
        out[p * R : (p + 1) * R, lanes] = total


def expand_grad_last(left, grad, out, looks):
    def one(half, _):
        lanes = lanes_of(half)
        rows = [grad[p * D3 : (p + 1) * D3, lanes] for p in range(D1 * D2)]
        for b in range(R):
            terms = [left[p * R + b : p * R + b + 1, lanes] * rows[p] for p in range(D1 * D2)]
            while len(terms) > 1:
                terms = [x + y for x, y in zip(terms[::2], terms[1::2])]
            out[b * D3 : (b + 1) * D3, lanes] = terms[0]
        return 0

    lax.fori_loop(0, looks // LANES, one, 0)


def expand_grad_first(grad_left, middle, out, looks):
    group = 4

    def block(step, _):
        lanes = lanes_of(step // (R // 8))
        base = (step % (R // 8)) * 8
        sums = [[] for _ in range(D1)]
        for extra in range(0, 8, group):
            totals = [[jnp.zeros((8, LANES), F32) for _ in range(group)] for _ in range(D1)]
            for part in range(D2 * R // 8):
                rows = [
                    middle[
                        pl.ds(pl.multiple_of((base + extra + a) * D2 * R, 8) + part * 8, 8), lanes
                    ]
                    for a in range(group)
                ]
                for i in range(D1):
                    weight = grad_left[i * D2 * R + part * 8 : i * D2 * R + part * 8 + 8, lanes]
                    for a in range(group):
                        totals[i][a] += weight * rows[a]
            for i in range(D1):
                sums[i] += [jnp.sum(totals[i][a], axis=0, keepdims=True) for a in range(group)]
        for i in range(D1):
            out[pl.ds(pl.multiple_of(i * R + base, 8), 8), lanes] = jnp.concatenate(sums[i], axis=0)
        return 0

    lax.fori_loop(0, (looks // LANES) * (R // 8), block, 0)


def local_kernel(
    sizes,
    place,
    bags,
    one,
    two,
    three,
    labels,
    core_one,
    core_two,
    core_three,
    dense,
    w_top,
    bias,
    w_out,
    parts,
    shared,
    first,
    middle,
    last,
    left,
    emb,
    grad,
    grad_left,
    grad_last,
    grad_first,
    total,
):
    n1, n2, n3, hid, samples, looks, nx, chunk = sizes
    width = D1 * D2 * D3
    hot_one = one_hot_rows(one[...], n1)
    hot_two = one_hot_rows(two[...], n2)
    hot_three = one_hot_rows(three[...], n3)
    hot_bag = one_hot_rows(bags[...], samples)
    first[...] = dot(core_one[...], hot_one, TN)
    found = dot(core_three[...], hot_three, TN)
    for half in range(looks // LANES):
        last[half] = found[:, half * LANES : (half + 1) * LANES]
    piece = 256
    for c in range(R * D2 * R // piece):
        middle[c * piece : (c + 1) * piece, :] = dot(
            core_two[:, c * piece : (c + 1) * piece], hot_two, TN
        )
    expand_left(first, middle, left, looks)
    expand_embedded(left, last, emb, looks)

    pooled = sum(dot(hot_bag, term, NT) for term in split(emb[...], 3))
    joined = jnp.concatenate([dense[...], pooled.astype(BF16)], axis=1)
    pre = nn(joined, w_top[...]) + bias[...]
    sig = jax.nn.sigmoid(pre)
    hidden = pre * sig
    weight = w_out[...]
    logit = jnp.sum(hidden * weight, axis=1, keepdims=True)
    grid = (samples, samples)
    same = lax.broadcasted_iota(jnp.int32, grid, 0) == lax.broadcasted_iota(jnp.int32, grid, 1)
    wanted = jnp.sum(jnp.where(same, labels[...].astype(F32), 0.0), axis=1, keepdims=True)
    dlogit = (jax.nn.sigmoid(logit) - wanted) / samples
    dpre = dlogit * weight * (sig * (1.0 + pre * (1.0 - sig)))
    low = dpre.astype(BF16)
    w_low = w_top[width : 2 * width, :]
    shared[0:samples, :] = dot(low, w_low, NT)
    for at, row in enumerate((bags, one, two, three)):
        for half in range(looks // LANES):
            spot = samples + at * (looks // LANES) + half
            shared[spot : spot + 1, :] = row[0:1, half * LANES : (half + 1) * LANES].astype(F32)

    turned = dot(w_low, low, NT)
    grad[...] = sum(nn(term, hot_bag) for term in split(turned))

    def back(half, _):
        expand_grad_left(grad, last.at[half], grad_left, lanes_of(half))
        return 0

    lax.fori_loop(0, looks // LANES, back, 0)
    expand_grad_last(left, grad, grad_last, looks)
    expand_grad_first(grad_left, middle, grad_first, looks)

    tops, ones, lasts, _ = sections(n1, n3, hid, 2 * width + 2)
    grad_weight = dot(joined, low, TN)
    grad_bias = jnp.sum(dpre, axis=0, keepdims=True)
    grad_output = jnp.sum(hidden * dlogit, axis=0, keepdims=True)
    total[...] = jnp.zeros(total.shape, F32)
    for half, start in enumerate(tops):
        cut = slice(half * LANES, (half + 1) * LANES)
        total[start : start + 2 * width, :] = grad_weight[:, cut]
        total[start + 2 * width : start + 2 * width + 1, :] = grad_bias[:, cut]
        total[start + 2 * width + 1 : start + 2 * width + 2, :] = grad_output[:, cut]
    total[ones : ones + n1, :] = sum(dot(hot_one, term, NT) for term in split(grad_first[...]))
    for half, start in enumerate(lasts):
        cut = slice(half * LANES, (half + 1) * LANES)
        total[start : start + n3, :] = sum(
            dot(hot_three, term, NT) for term in split(grad_last[cut, :])
        )

    def lay(chunk_id, _):
        key = chunk_id ^ place[0]
        spot = (key % 2) * (nx // 2) + key // 2
        parts[spot] = total[pl.ds(pl.multiple_of(chunk_id * chunk, 8), chunk), :]
        return 0

    lax.fori_loop(0, nx, lay, 0)


def previous(x, amount):
    rows = x.shape[0]
    down, across = divmod(amount, LANES)
    if across:
        x = pltpu.roll(x, LANES - across, axis=1)
        lane = lax.broadcasted_iota(jnp.int32, x.shape, 1)
        x = jnp.where(lane < LANES - across, x, pltpu.roll(x, rows - 1, axis=0))
    if down:
        x = pltpu.roll(x, rows - down, axis=0)
    return x


def owner_kernel(sizes, row_start, table, core_one, core_three, window, fields, turned, first, last, grad, grad_left):
    n1, n3, samples, looks, height, blocks, rows = sizes
    per = looks // LANES
    low_row = row_start[0]
    names = []
    for at in range(4):
        pieces = [
            table[k * height + samples + at * per : k * height + samples + (at + 1) * per, :]
            for k in range(blocks)
        ]
        names.append(jnp.concatenate(pieces, axis=0))
    bag, one, two, three = names
    total = blocks * per
    line = lax.broadcasted_iota(jnp.int32, (total, LANES), 0)
    flat = line * LANES + lax.broadcasted_iota(jnp.int32, (total, LANES), 1)
    sample = bag + ((line // per) * height).astype(F32)
    local = two - low_row.astype(F32)
    inside = (local >= 0.0) & (local < float(rows))
    mask = jnp.where(inside, 1.0, 0.0).astype(BF16)
    upper = lax.broadcasted_iota(jnp.int32, (LANES, LANES), 0) < lax.broadcasted_iota(
        jnp.int32, (LANES, LANES), 1
    )
    lower = lax.broadcasted_iota(jnp.int32, (total, total), 1) < lax.broadcasted_iota(
        jnp.int32, (total, total), 0
    )
    within = nn(mask, jnp.where(upper, 1.0, 0.0).astype(BF16))
    above = jnp.sum(nn(jnp.where(lower, 1.0, 0.0).astype(BF16), mask), axis=1, keepdims=True)
    rank = (within + above).astype(jnp.int32)
    count = jnp.sum(mask.astype(F32)).astype(jnp.int32)
    way = jnp.where(inside, flat - rank, 0)
    held = [sample, one, local, three, jnp.where(inside, 1.0, 0.0)]
    size = 1
    while size < total * LANES:
        moved = previous(way, size)
        take = ((moved & size) != 0) & (flat < total * LANES - size)
        leave = (way & size) != 0
        live = previous(held[4], size)
        take = take & (live > 0.0)
        held = [
            jnp.where(take, previous(x, size) if x is not held[4] else live, jnp.where(leave, 0.0, x))
            for x in held
        ]
        way = jnp.where(take, moved - size, jnp.where(leave, 0, way))
        size *= 2
    for at, x in enumerate(held):
        fields[at] = x

    pieces, _, piece = turned.shape

    def flip(c, _):
        flipped = table[pl.ds(pl.multiple_of(c * piece, 8), piece), :].T
        for at, term in enumerate(split(flipped)):
            turned[c, at * LANES : (at + 1) * LANES, :] = term
        return 0

    lax.fori_loop(0, pieces, flip, 0)

    window[...] = jnp.zeros(window.shape, F32)
    lanes = pl.ds(0, LANES)

    def some(step, _):
        rows_at = pl.ds(pl.multiple_of((step // 8) * 8, 8), 8)
        pick = lax.broadcasted_iota(jnp.int32, (8, LANES), 0) == step % 8
        values = [
            jnp.sum(jnp.where(pick, fields[at, rows_at, :], 0.0), axis=0, keepdims=True)
            for at in range(5)
        ]
        live = values[4] > 0.0
        at = jnp.where(live, values[0], -1.0).astype(jnp.int32)
        first[...] = dot(core_one[...], one_hot_rows(values[1].astype(jnp.int32), n1), TN)
        last[...] = dot(core_three[...], one_hot_rows(values[3].astype(jnp.int32), n3), TN)
        grad[...] = jnp.zeros(grad.shape, F32)

        def find(c, _):
            found = nn(turned[c], one_hot_rows(at - c * piece, piece))
            grad[...] += found[0:LANES] + found[LANES : 2 * LANES]
            return 0

        lax.fori_loop(0, pieces, find, 0, unroll=pieces < 16)
        expand_grad_left(grad, last, grad_left, lanes)
        spot = jnp.where(live, values[2], -1.0).astype(jnp.int32)
        for i in range(D1):
            part = first[i * R : (i + 1) * R, :]
            stacked = jnp.concatenate(
                [jnp.where(spot == r, part, 0.0).astype(BF16) for r in range(rows)], axis=0
            )
            for term in split(grad_left[i * D2 * R : (i + 1) * D2 * R, :]):
                window[...] += dot(stacked, term, NT)
        return 0

    lax.fori_loop(0, (count + LANES - 1) // LANES, some, 0)


def final_kernel(sizes, place, chunks, window, top, core, total, source):
    n1, n3, hid, nx, chunk, rows, out_rows = sizes
    width = D1 * D2 * D3

    def lay(chunk_id, _):
        key = chunk_id ^ place[0]
        spot = (key % 2) * (nx // 2) + key // 2
        total[pl.ds(pl.multiple_of(chunk_id * chunk, 8), chunk), :] = chunks[spot]
        return 0

    lax.fori_loop(0, nx, lay, 0)
    top_rows = 2 * width + 2
    tops, ones, lasts, _ = sections(n1, n3, hid, top_rows)
    for half, start in enumerate(tops):
        top[:, half * LANES : (half + 1) * LANES] = total[start : start + top_rows, :]
    source[0:n1, :] = total[ones : ones + n1, :]
    wide = rows * R
    source[n1 : n1 + wide, :] = window[...]
    for half, start in enumerate(lasts):
        source[pl.ds(n1 + wide + half, n3, stride=len(lasts)), :] = total[start : start + n3, :]
    upper = source[pl.ds(place[1], out_rows), :]
    lower = source[pl.ds(place[1] + 1, out_rows), :]
    shift = place[2]
    turn = (LANES - shift) % LANES
    lane = lax.broadcasted_iota(jnp.int32, upper.shape, 1)
    core[...] = jnp.where(
        lane < LANES - shift, pltpu.roll(upper, turn, axis=1), pltpu.roll(lower, turn, axis=1)
    )


def xor_permute(x, axis, size, mask):
    return lax.ppermute(x, axis, [(j, j ^ mask) for j in range(size)])


def tree(terms):
    while len(terms) > 1:
        pairs = [x + y for x, y in zip(terms[::2], terms[1::2])]
        terms = pairs + ([terms[-1]] if len(terms) % 2 else [])
    return terms[0]


def gather_all(x, axis, size, masks):
    return [x] + [xor_permute(x, axis, size, mask) for mask in masks]


def per_device(nx, ny, core_one, core_two, core_three, dense_rows, w_top, bias_top, w_out, labels, bag_ids, digit_one, digit_two, digit_three):
    n1, n2, n3 = core_one.shape[0], core_two.shape[0], core_three.shape[0]
    hid = w_top.shape[1]
    samples = dense_rows.shape[0]
    looks = bag_ids.shape[1]
    width = D1 * D2 * D3
    per = looks // LANES
    blocks = nx * ny
    gx = lax.axis_index("gx")
    gy = lax.axis_index("gy")
    _, _, _, rows_all = sections(n1, n3, hid, 2 * width + 2)
    chunk = up(up(rows_all, nx) // nx, 8)
    height = up(samples + 4 * per, 8)

    vmem = pl.BlockSpec(memory_space=pltpu.VMEM)
    smem = pl.BlockSpec(memory_space=pltpu.SMEM)
    params = pltpu.CompilerParams(vmem_limit_bytes=VMEM_LIMIT)
    sizes = (n1, n2, n3, hid, samples, looks, nx, chunk)
    parts, shared = pl.pallas_call(
        functools.partial(local_kernel, sizes),
        out_shape=(
            jax.ShapeDtypeStruct((nx, chunk, LANES), F32),
            jax.ShapeDtypeStruct((height, LANES), F32),
        ),
        in_specs=[smem] + [vmem] * 12,
        out_specs=(vmem, vmem),
        scratch_shapes=[
            pltpu.VMEM((D1 * R, looks), F32),
            pltpu.VMEM((R * D2 * R, looks), F32),
            pltpu.VMEM((looks // LANES, R * D3, LANES), F32),
            pltpu.VMEM((D1 * D2 * R, looks), F32),
            pltpu.VMEM((width, looks), F32),
            pltpu.VMEM((width, looks), F32),
            pltpu.VMEM((D1 * D2 * R, looks), F32),
            pltpu.VMEM((R * D3, looks), F32),
            pltpu.VMEM((D1 * R, looks), F32),
            pltpu.VMEM((nx * chunk, LANES), F32),
        ],
        compiler_params=params,
        cost_estimate=pl.CostEstimate(flops=4_000_000_000, bytes_accessed=4_000_000, transcendentals=0),
        name="local",
    )(
        gx.reshape(1),
        bag_ids,
        digit_one,
        digit_two,
        digit_three,
        labels.reshape(1, samples),
        core_one,
        core_two,
        core_three,
        dense_rows,
        w_top,
        bias_top.reshape(1, hid),
        w_out.reshape(1, hid),
    )

    table = jnp.concatenate(gather_all(shared, "gy", ny, range(1, ny)), axis=0)
    table = jnp.concatenate(gather_all(table, "gx", nx, [2 * k for k in range(1, nx // 2)]), axis=0)
    table = jnp.concatenate([table, xor_permute(table, "gx", nx, 1)], axis=0)

    half = parts.reshape(2, nx // 2, chunk, LANES)
    half = half[0] + xor_permute(half[1], "gx", nx, 1)
    mine = tree(
        [half[0]] + [xor_permute(half[k], "gx", nx, 2 * k) for k in range(1, nx // 2)]
    )
    mine = tree(gather_all(mine, "gy", ny, range(1, ny)))
    chips = jnp.stack(gather_all(mine, "gx", nx, [2 * k for k in range(1, nx // 2)]))
    chunks = jnp.concatenate([chips, xor_permute(chips, "gx", nx, 1)], axis=0)

    share = (core_one.size + core_two.size + core_three.size) // blocks
    length = R * D2 * R
    rows = min((share + 2 * length - 2) // length, n2)
    begin = (gx * ny + gy) * share - core_one.size
    row_start = jnp.clip(begin // length, 0, n2 - rows).astype(jnp.int32)
    window = pl.pallas_call(
        functools.partial(owner_kernel, (n1, n3, samples, looks, height, blocks, rows)),
        out_shape=jax.ShapeDtypeStruct((rows * R, LANES), F32),
        in_specs=[smem] + [vmem] * 3,
        out_specs=vmem,
        scratch_shapes=[
            pltpu.VMEM((5, blocks * per, LANES), F32),
            pltpu.VMEM((blocks // 8, 2 * LANES, 8 * height), BF16),
            pltpu.VMEM((D1 * R, LANES), F32),
            pltpu.VMEM((R * D3, LANES), F32),
            pltpu.VMEM((width, LANES), F32),
            pltpu.VMEM((D1 * D2 * R, LANES), F32),
        ],
        compiler_params=params,
        cost_estimate=pl.CostEstimate(flops=4_000_000_000, bytes_accessed=2_000_000, transcendentals=0),
        name="owner",
    )(row_start.reshape(1), table, core_one, core_three)

    out_rows = up(share, LANES) // LANES
    start = core_one.size + begin - row_start * length
    place = jnp.stack([gx, start // LANES, start % LANES]).astype(jnp.int32)
    source_rows = up(n1 + rows * R + n3 * (R * D3 // LANES) + out_rows, 8)
    top, core = pl.pallas_call(
        functools.partial(final_kernel, (n1, n3, hid, nx, chunk, rows, out_rows)),
        out_shape=(
            jax.ShapeDtypeStruct((2 * width + 2, hid), F32),
            jax.ShapeDtypeStruct((out_rows, LANES), F32),
        ),
        in_specs=[smem, vmem, vmem],
        out_specs=(vmem, vmem),
        scratch_shapes=[
            pltpu.VMEM((nx * chunk, LANES), F32),
            pltpu.VMEM((source_rows, LANES), F32),
        ],
        compiler_params=params,
        name="final",
    )(place, chunks, window)
    return core.reshape(-1)[:share], top


def solution(mesh):
    both = ("gx", "gy")
    return jax.shard_map(
        functools.partial(per_device, mesh.shape["gx"], mesh.shape["gy"]),
        mesh=mesh,
        in_specs=(
            P(),
            P(),
            P(),
            P(both, None),
            P(),
            P(),
            P(),
            P(both),
            P(both, None),
            P(both, None),
            P(both, None),
            P(both, None),
        ),
        out_specs=(P(both), P()),
        check_vma=False,
    )
```

```python
import functools

import jax
import jax.numpy as jnp
from jax import lax
from jax.experimental import pallas as pl
from jax.experimental.pallas import tpu as pltpu
from jax.sharding import PartitionSpec as P


D1 = 4
D2 = 4
D3 = 8
R = 32
LANES = 128
F32 = jnp.float32
BF16 = jnp.bfloat16
TN = (((0,), (0,)), ((), ()))
NT = (((1,), (1,)), ((), ()))
VMEM_LIMIT = 60 * 1024 * 1024


def up(value, step):
    return -(-value // step) * step


def dot(a, b, dims):
    return lax.dot_general(a, b, dims, preferred_element_type=F32)


def nn(a, b):
    return jnp.dot(a, b, preferred_element_type=F32)


def split(x, count=2):
    terms = []
    for _ in range(count):
        terms.append(x.astype(BF16))
        x = x - terms[-1].astype(F32)
    return terms


def one_hot_rows(row, count):
    grid = lax.broadcasted_iota(jnp.int32, (count, row.shape[1]), 0)
    return jnp.where(grid == row, 1.0, 0.0).astype(BF16)


def sections(n1, n3, hid, top_rows):
    halves = hid // LANES
    top = [part * up(top_rows, 8) for part in range(halves)]
    ones = halves * up(top_rows, 8)
    wide = (R * D3) // LANES
    lasts = [ones + up(n1, 8) + part * up(n3, 8) for part in range(wide)]
    return top, ones, lasts, lasts[-1] + up(n3, 8)


def expand_left(first, middle, left, looks):
    def block(step, _):
        lanes = pl.ds(pl.multiple_of((step // 4) * LANES, LANES), LANES)
        base = (step % 4) * R
        totals = [jnp.zeros((R, LANES), F32) for _ in range(D1)]
        for a in range(R):
            rows = middle[pl.ds(a * D2 * R + base, R), lanes]
            for i in range(D1):
                totals[i] += first[i * R + a : i * R + a + 1, lanes] * rows
        for i in range(D1):
            left[pl.ds(i * D2 * R + base, R), lanes] = totals[i]
        return 0

    lax.fori_loop(0, (looks // LANES) * D2, block, 0)


def lanes_of(half):
    return pl.ds(pl.multiple_of(half * LANES, LANES), LANES)


def expand_embedded(left, last, out, looks):
    def one(half, _):
        lanes = lanes_of(half)
        totals = [jnp.zeros((D3, LANES), F32) for _ in range(D1 * D2)]
        for b in range(R):
            rows = last[half, b * D3 : (b + 1) * D3, :]
            for p in range(D1 * D2):
                totals[p] += left[p * R + b : p * R + b + 1, lanes] * rows
        for p in range(D1 * D2):
            out[p * D3 : (p + 1) * D3, lanes] = totals[p]
        return 0

    lax.fori_loop(0, looks // LANES, one, 0)


def expand_grad_left(grad, last, out, lanes):
    turned = [last[pl.ds(d, R, stride=D3), :] for d in range(D3)]
    for p in range(D1 * D2):
        total = jnp.zeros((R, LANES), F32)
        for d in range(D3):
            total += grad[p * D3 + d : p * D3 + d + 1, lanes] * turned[d]
        out[p * R : (p + 1) * R, lanes] = total


def expand_grad_last(left, grad, out, looks):
    def one(half, _):
        lanes = lanes_of(half)
        rows = [grad[p * D3 : (p + 1) * D3, lanes] for p in range(D1 * D2)]
        for b in range(R):
            terms = [left[p * R + b : p * R + b + 1, lanes] * rows[p] for p in range(D1 * D2)]
            while len(terms) > 1:
                terms = [x + y for x, y in zip(terms[::2], terms[1::2])]
            out[b * D3 : (b + 1) * D3, lanes] = terms[0]
        return 0

    lax.fori_loop(0, looks // LANES, one, 0)


def expand_grad_first(grad_left, middle, out, looks):
    group = 8

    def block(half, _):
        lanes = lanes_of(half)
        for base in range(0, R, group):
            totals = [[None] * group for _ in range(D1)]
            for part in range(0, D2 * R, 8):
                rows = [
                    middle[(base + a) * D2 * R + part : (base + a) * D2 * R + part + 8, lanes]
                    for a in range(group)
                ]
                for i in range(D1):
                    weight = grad_left[i * D2 * R + part : i * D2 * R + part + 8, lanes]
                    for a in range(group):
                        term = weight * rows[a]
                        totals[i][a] = totals[i][a] + term if part else term
            for i in range(D1):
                for a in range(group):
                    out[half, pl.ds(i * R + base + a, 8, stride=D1 * R), :] = totals[i][a]
        return 0

    lax.fori_loop(0, looks // LANES, block, 0)


def local_kernel(
    sizes,
    bags,
    one,
    two,
    three,
    labels,
    core_one,
    core_two,
    core_three,
    dense,
    w_top,
    bias,
    w_out,
    keep,
    send,
    shared,
    first,
    middle,
    last,
    left,
    emb,
    grad,
    grad_left,
    grad_last,
    grad_first,
    total,
):
    n1, n2, n3, hid, samples, looks, nx, chunk = sizes
    width = D1 * D2 * D3
    hot_one = one_hot_rows(one[...], n1)
    hot_two = one_hot_rows(two[...], n2)
    hot_three = one_hot_rows(three[...], n3)
    hot_bag = one_hot_rows(bags[...], samples)
    first[...] = dot(core_one[...], hot_one, TN)
    found = dot(core_three[...], hot_three, TN)
    for half in range(looks // LANES):
        last[half] = found[:, half * LANES : (half + 1) * LANES]
    piece = 256
    for c in range(R * D2 * R // piece):
        middle[c * piece : (c + 1) * piece, :] = dot(
            core_two[:, c * piece : (c + 1) * piece], hot_two, TN
        )
    expand_left(first, middle, left, looks)
    expand_embedded(left, last, emb, looks)

    pooled = sum(dot(hot_bag, term, NT) for term in split(emb[...], 3))
    joined = jnp.concatenate([dense[...], pooled.astype(BF16)], axis=1)
    pre = nn(joined, w_top[...]) + bias[...]
    sig = jax.nn.sigmoid(pre)
    hidden = pre * sig
    weight = w_out[...]
    logit = jnp.sum(hidden * weight, axis=1, keepdims=True)
    grid = (samples, samples)
    same = lax.broadcasted_iota(jnp.int32, grid, 0) == lax.broadcasted_iota(jnp.int32, grid, 1)
    wanted = jnp.sum(jnp.where(same, labels[...].astype(F32), 0.0), axis=1, keepdims=True)
    dlogit = (jax.nn.sigmoid(logit) - wanted) / samples
    dpre = dlogit * weight * (sig * (1.0 + pre * (1.0 - sig)))
    low = dpre.astype(BF16)
    w_low = w_top[width : 2 * width, :]
    shared[0:samples, :] = dot(low, w_low, NT)
    for at, row in enumerate((bags, one, two, three)):
        for half in range(looks // LANES):
            spot = samples + at * (looks // LANES) + half
            shared[spot : spot + 1, :] = row[0:1, half * LANES : (half + 1) * LANES].astype(F32)

    turned = dot(w_low, low, NT)
    grad[...] = sum(nn(term, hot_bag) for term in split(turned))

    def back(half, _):
        expand_grad_left(grad, last.at[half], grad_left, lanes_of(half))
        return 0

    lax.fori_loop(0, looks // LANES, back, 0)
    expand_grad_last(left, grad, grad_last, looks)
    expand_grad_first(grad_left, middle, grad_first, looks)

    tops, ones, lasts, _ = sections(n1, n3, hid, 2 * width + 2)
    grad_weight = dot(joined, low, TN)
    grad_bias = jnp.sum(dpre, axis=0, keepdims=True)
    grad_output = jnp.sum(hidden * dlogit, axis=0, keepdims=True)
    total[...] = jnp.zeros(total.shape, F32)
    for half, start in enumerate(tops):
        cut = slice(half * LANES, (half + 1) * LANES)
        total[start : start + 2 * width, :] = grad_weight[:, cut]
        total[start + 2 * width : start + 2 * width + 1, :] = grad_bias[:, cut]
        total[start + 2 * width + 1 : start + 2 * width + 2, :] = grad_output[:, cut]
    wide = jnp.concatenate([grad_first[half] for half in range(looks // LANES)], axis=1)
    found = sum(dot(hot_one, term, NT) for term in split(wide))
    total[ones : ones + n1, :] = tree([found[:, at * LANES : (at + 1) * LANES] for at in range(8)])
    for half, start in enumerate(lasts):
        cut = slice(half * LANES, (half + 1) * LANES)
        total[start : start + n3, :] = sum(
            dot(hot_three, term, NT) for term in split(grad_last[cut, :])
        )

    gx = lax.axis_index("gx")
    for key in range(nx):
        target = keep if key % 2 == 0 else send
        target[key // 2] = total[pl.ds(pl.multiple_of((gx ^ key) * chunk, 8), chunk), :]


def previous(x, amount):
    rows = x.shape[0]
    down, across = divmod(amount, LANES)
    if across:
        x = pltpu.roll(x, LANES - across, axis=1)
        lane = lax.broadcasted_iota(jnp.int32, x.shape, 1)
        x = jnp.where(lane < LANES - across, x, pltpu.roll(x, rows - 1, axis=0))
    if down:
        x = pltpu.roll(x, rows - down, axis=0)
    return x


def spans(index, share, n1, n2):
    length = R * D2 * R
    rows = min((share + 2 * length - 2) // length, n2)
    begin = index * share - n1 * D1 * R
    row = jnp.minimum(lax.div(jnp.maximum(begin, 0), length), n2 - rows)
    return rows, begin, row


def owner_kernel(sizes, index, table, core_one, core_three, window, fields, turned, core_first, core_last, first, last, grad, grad_left):
    n1, n2, n3, share, samples, looks, height, blocks = sizes
    per = looks // LANES
    rows, _, low_row = spans(index[0], share, n1, n2)
    core_first[...] = core_one[...].astype(F32).T.astype(BF16)
    core_last[...] = core_three[...].astype(F32).T.astype(BF16)
    names = []
    for at in range(4):
        pieces = [
            table[k * height + samples + at * per : k * height + samples + (at + 1) * per, :]
            for k in range(blocks)
        ]
        names.append(jnp.concatenate(pieces, axis=0))
    bag, one, two, three = names
    total = blocks * per
    line = lax.broadcasted_iota(jnp.int32, (total, LANES), 0)
    flat = line * LANES + lax.broadcasted_iota(jnp.int32, (total, LANES), 1)
    sample = bag + ((line // per) * height).astype(F32)
    local = two - low_row.astype(F32)
    inside = (local >= 0.0) & (local < float(rows))
    mask = jnp.where(inside, 1.0, 0.0).astype(BF16)
    upper = lax.broadcasted_iota(jnp.int32, (LANES, LANES), 0) < lax.broadcasted_iota(
        jnp.int32, (LANES, LANES), 1
    )
    lower = lax.broadcasted_iota(jnp.int32, (total, total), 1) < lax.broadcasted_iota(
        jnp.int32, (total, total), 0
    )
    within = nn(mask, jnp.where(upper, 1.0, 0.0).astype(BF16))
    above = jnp.sum(nn(jnp.where(lower, 1.0, 0.0).astype(BF16), mask), axis=1, keepdims=True)
    rank = (within + above).astype(jnp.int32)
    count = jnp.sum(mask.astype(F32)).astype(jnp.int32)
    way = jnp.where(inside, flat - rank, 0)
    held = [sample, one, local, three, jnp.where(inside, 1.0, 0.0)]
    size = 1
    while size < total * LANES:
        moved = previous(way, size)
        take = ((moved & size) != 0) & (flat < total * LANES - size)
        leave = (way & size) != 0
        live = previous(held[4], size)
        take = take & (live > 0.0)
        held = [
            jnp.where(take, previous(x, size) if x is not held[4] else live, jnp.where(leave, 0.0, x))
            for x in held
        ]
        way = jnp.where(take, moved - size, jnp.where(leave, 0, way))
        size *= 2
    for at, x in enumerate(held):
        fields[at] = x

    pieces, _, piece = turned.shape

    def flip(c, _):
        flipped = table[pl.ds(pl.multiple_of(c * piece, 8), piece), :].T
        for at, term in enumerate(split(flipped)):
            turned[c, at * LANES : (at + 1) * LANES, :] = term
        return 0

    lax.fori_loop(0, pieces, flip, 0)

    window[...] = jnp.zeros(window.shape, F32)
    lanes = pl.ds(0, LANES)

    def some(step, _):
        rows_at = pl.ds(pl.multiple_of((step // 8) * 8, 8), 8)
        pick = lax.broadcasted_iota(jnp.int32, (8, LANES), 0) == step % 8
        values = [
            jnp.sum(jnp.where(pick, fields[at, rows_at, :], 0.0), axis=0, keepdims=True)
            for at in range(5)
        ]
        live = values[4] > 0.0
        at = jnp.where(live, values[0], -1.0).astype(jnp.int32)
        first[...] = nn(core_first[...], one_hot_rows(values[1].astype(jnp.int32), n1))
        last[...] = nn(core_last[...], one_hot_rows(values[3].astype(jnp.int32), n3))
        grad[...] = jnp.zeros(grad.shape, F32)

        def find(c, _):
            found = nn(turned[c], one_hot_rows(at - c * piece, piece))
            grad[...] += found[0:LANES] + found[LANES : 2 * LANES]
            return 0

        lax.fori_loop(0, pieces, find, 0, unroll=pieces < 16)
        expand_grad_left(grad, last, grad_left, lanes)
        spot = jnp.where(live, values[2], -1.0).astype(jnp.int32)
        here = [spot == r for r in range(rows)]
        stacked = []
        for i in range(D1):
            part = first[i * R : (i + 1) * R, :]
            picked = [jnp.where(at_row, part, 0.0) for at_row in here]
            stacked.append(jnp.concatenate(picked, axis=0).astype(BF16))
        terms = [split(grad_left[i * D2 * R : (i + 1) * D2 * R, :]) for i in range(D1)]
        sides = [jnp.concatenate([term[at] for term in terms], axis=1) for at in range(2)]
        found = dot(jnp.concatenate(stacked, axis=1), jnp.concatenate(sides, axis=0), NT)
        window[...] += found[:, 0 : D2 * R] + found[:, D2 * R : 2 * D2 * R]
        return 0

    lax.fori_loop(0, (count + LANES - 1) // LANES, some, 0)


def final_kernel(sizes, index, chips, others, window, top, core, total, source, sems):
    n1, n2, n3, hid, ny, share, nx, chunk, out_rows = sizes
    width = D1 * D2 * D3
    gx = lax.axis_index("gx")
    copies = []
    for key in range(nx):
        origin = (chips if key % 2 == 0 else others).at[key // 2]
        into = total.at[pl.ds(pl.multiple_of((gx ^ key) * chunk, 8), chunk), :]
        copies.append(pltpu.make_async_copy(origin, into, sems.at[key]))
    for copy in copies:
        copy.start()
    for copy in copies:
        copy.wait()
    rows, begin, row = spans(index[0], share, n1, n2)
    start = n1 * D1 * R + begin - row * R * D2 * R
    top_rows = 2 * width + 2
    tops, ones, lasts, _ = sections(n1, n3, hid, top_rows)
    for half, at in enumerate(tops):
        top[:, half * LANES : (half + 1) * LANES] = total[at : at + top_rows, :]
    source[0:n1, :] = total[ones : ones + n1, :]
    wide = rows * R
    source[n1 : n1 + wide, :] = window[...]
    for half, at in enumerate(lasts):
        source[pl.ds(n1 + wide + half, n3, stride=len(lasts)), :] = total[at : at + n3, :]
    upper = source[pl.ds(lax.div(start, LANES), out_rows), :]
    lower = source[pl.ds(lax.div(start, LANES) + 1, out_rows), :]
    shift = lax.rem(start, LANES)
    turn = (LANES - shift) % LANES
    lane = lax.broadcasted_iota(jnp.int32, upper.shape, 1)
    core[...] = jnp.where(
        lane < LANES - shift, pltpu.roll(upper, turn, axis=1), pltpu.roll(lower, turn, axis=1)
    )


def xor_permute(x, axis, size, mask):
    return lax.ppermute(x, axis, [(j, j ^ mask) for j in range(size)])


def tree(terms):
    while len(terms) > 1:
        pairs = [x + y for x, y in zip(terms[::2], terms[1::2])]
        terms = pairs + ([terms[-1]] if len(terms) % 2 else [])
    return terms[0]


def gather_all(x, axis, size, masks):
    return [x] + [xor_permute(x, axis, size, mask) for mask in masks]


def per_device(nx, ny, core_one, core_two, core_three, dense_rows, w_top, bias_top, w_out, labels, bag_ids, digit_one, digit_two, digit_three):
    n1, n2, n3 = core_one.shape[0], core_two.shape[0], core_three.shape[0]
    hid = w_top.shape[1]
    samples = dense_rows.shape[0]
    looks = bag_ids.shape[1]
    width = D1 * D2 * D3
    per = looks // LANES
    blocks = nx * ny
    _, _, _, rows_all = sections(n1, n3, hid, 2 * width + 2)
    chunk = up(up(rows_all, nx) // nx, 8)
    height = up(samples + 4 * per, 8)

    vmem = pl.BlockSpec(memory_space=pltpu.VMEM)
    smem = pl.BlockSpec(memory_space=pltpu.SMEM)
    index = (lax.axis_index("gx") * ny + lax.axis_index("gy")).astype(jnp.int32).reshape(1)
    params = pltpu.CompilerParams(vmem_limit_bytes=VMEM_LIMIT)
    sizes = (n1, n2, n3, hid, samples, looks, nx, chunk)
    keep, send, shared = pl.pallas_call(
        functools.partial(local_kernel, sizes),
        out_shape=(
            jax.ShapeDtypeStruct((nx // 2, chunk, LANES), F32),
            jax.ShapeDtypeStruct((nx // 2, chunk, LANES), F32),
            jax.ShapeDtypeStruct((height, LANES), F32),
        ),
        in_specs=[vmem] * 12,
        out_specs=(vmem, vmem, vmem),
        scratch_shapes=[
            pltpu.VMEM((D1 * R, looks), F32),
            pltpu.VMEM((R * D2 * R, looks), F32),
            pltpu.VMEM((looks // LANES, R * D3, LANES), F32),
            pltpu.VMEM((D1 * D2 * R, looks), F32),
            pltpu.VMEM((width, looks), F32),
            pltpu.VMEM((width, looks), F32),
            pltpu.VMEM((D1 * D2 * R, looks), F32),
            pltpu.VMEM((R * D3, looks), F32),
            pltpu.VMEM((looks // LANES, 8 * D1 * R, LANES), F32),
            pltpu.VMEM((nx * chunk, LANES), F32),
        ],
        compiler_params=params,
        cost_estimate=pl.CostEstimate(flops=4_000_000_000, bytes_accessed=4_000_000, transcendentals=0),
        name="local",
    )(
        bag_ids,
        digit_one,
        digit_two,
        digit_three,
        labels.reshape(1, samples),
        core_one,
        core_two,
        core_three,
        dense_rows,
        w_top,
        bias_top.reshape(1, hid),
        w_out.reshape(1, hid),
    )

    across = [2 * k for k in range(1, nx // 2)]
    with jax.named_scope("pair_sum"):
        half = keep + xor_permute(send, "gx", nx, 1)
    with jax.named_scope("table_z"):
        table = jnp.concatenate(gather_all(shared, "gy", ny, range(1, ny)), axis=0)
    with jax.named_scope("chip_sum"):
        mine = tree([half[0]] + [xor_permute(half[k // 2], "gx", nx, k) for k in across])
    with jax.named_scope("table_xy"):
        mask = 2
        while mask < nx:
            table = jnp.concatenate([table, xor_permute(table, "gx", nx, mask)], axis=0)
            mask *= 2
    with jax.named_scope("z_sum"):
        mine = tree(gather_all(mine, "gy", ny, range(1, ny)))
    mine, table = lax.optimization_barrier((mine, table))
    with jax.named_scope("table_pair"):
        table = jnp.concatenate([table, xor_permute(table, "gx", nx, 1)], axis=0)
    with jax.named_scope("chip_all"):
        chips = jnp.stack(gather_all(mine, "gx", nx, across))
    with jax.named_scope("pair_all"):
        others = xor_permute(chips, "gx", nx, 1)

    share = (core_one.size + core_two.size + core_three.size) // blocks
    length = R * D2 * R
    rows = min((share + 2 * length - 2) // length, n2)
    window = pl.pallas_call(
        functools.partial(owner_kernel, (n1, n2, n3, share, samples, looks, height, blocks)),
        out_shape=jax.ShapeDtypeStruct((rows * R, LANES), F32),
        in_specs=[smem] + [vmem] * 3,
        out_specs=vmem,
        scratch_shapes=[
            pltpu.VMEM((5, blocks * per, LANES), F32),
            pltpu.VMEM((blocks // 8, 2 * LANES, 8 * height), BF16),
            pltpu.VMEM((D1 * R, n1), BF16),
            pltpu.VMEM((R * D3, n3), BF16),
            pltpu.VMEM((D1 * R, LANES), F32),
            pltpu.VMEM((R * D3, LANES), F32),
            pltpu.VMEM((width, LANES), F32),
            pltpu.VMEM((D1 * D2 * R, LANES), F32),
        ],
        compiler_params=params,
        cost_estimate=pl.CostEstimate(flops=4_000_000_000, bytes_accessed=2_000_000, transcendentals=0),
        name="owner",
    )(index, table, core_one, core_three)

    out_rows = up(share, LANES) // LANES
    source_rows = up(n1 + rows * R + n3 * (R * D3 // LANES) + out_rows, 8)
    top, core = pl.pallas_call(
        functools.partial(final_kernel, (n1, n2, n3, hid, ny, share, nx, chunk, out_rows)),
        out_shape=(
            jax.ShapeDtypeStruct((2 * width + 2, hid), F32),
            jax.ShapeDtypeStruct((out_rows, LANES), F32),
        ),
        in_specs=[smem] + [pl.BlockSpec(memory_space=pl.ANY)] * 2 + [vmem],
        out_specs=(vmem, vmem),
        scratch_shapes=[
            pltpu.VMEM((nx * chunk, LANES), F32),
            pltpu.VMEM((source_rows, LANES), F32),
            pltpu.SemaphoreType.DMA((nx,)),
        ],
        compiler_params=params,
        name="final",
    )(index, chips, others, window)
    return core.reshape(-1)[:share], top


def solution(mesh):
    both = ("gx", "gy")
    return jax.shard_map(
        functools.partial(per_device, mesh.shape["gx"], mesh.shape["gy"]),
        mesh=mesh,
        in_specs=(
            P(),
            P(),
            P(),
            P(both, None),
            P(),
            P(),
            P(),
            P(both),
            P(both, None),
            P(both, None),
            P(both, None),
            P(both, None),
        ),
        out_specs=(P(both), P()),
        check_vma=False,
    )
```

```python
import functools

import jax
import jax.numpy as jnp
from jax import lax
from jax.experimental import pallas as pl
from jax.experimental.pallas import tpu as pltpu
from jax.sharding import PartitionSpec as P


D1 = 4
D2 = 4
D3 = 8
R = 32
LANES = 128
F32 = jnp.float32
BF16 = jnp.bfloat16
TN = (((0,), (0,)), ((), ()))
NT = (((1,), (1,)), ((), ()))
VMEM_LIMIT = 60 * 1024 * 1024


def up(value, step):
    return -(-value // step) * step


def dot(a, b, dims):
    return lax.dot_general(a, b, dims, preferred_element_type=F32)


def nn(a, b):
    return jnp.dot(a, b, preferred_element_type=F32)


def split(x, count=2):
    terms = []
    for _ in range(count):
        terms.append(x.astype(BF16))
        x = x - terms[-1].astype(F32)
    return terms


def one_hot_rows(row, count):
    grid = lax.broadcasted_iota(jnp.int32, (count, row.shape[1]), 0)
    return jnp.where(grid == row, 1.0, 0.0).astype(BF16)


def sections(n1, n3, hid, top_rows):
    halves = hid // LANES
    top = [part * up(top_rows, 8) for part in range(halves)]
    ones = halves * up(top_rows, 8)
    wide = (R * D3) // LANES
    lasts = [ones + up(n1, 8) + part * up(n3, 8) for part in range(wide)]
    return top, ones, lasts, lasts[-1] + up(n3, 8)


def expand_left(first, middle, left, looks):
    def block(step, _):
        lanes = pl.ds(pl.multiple_of((step // 4) * LANES, LANES), LANES)
        base = (step % 4) * R
        totals = [jnp.zeros((R, LANES), F32) for _ in range(D1)]
        for a in range(R):
            rows = middle[pl.ds(a * D2 * R + base, R), lanes]
            for i in range(D1):
                totals[i] += first[i * R + a : i * R + a + 1, lanes] * rows
        for i in range(D1):
            left[pl.ds(i * D2 * R + base, R), lanes] = totals[i]
        return 0

    lax.fori_loop(0, (looks // LANES) * D2, block, 0)


def lanes_of(half):
    return pl.ds(pl.multiple_of(half * LANES, LANES), LANES)


def expand_embedded(left, last, out, looks):
    def one(half, _):
        lanes = lanes_of(half)
        totals = [jnp.zeros((D3, LANES), F32) for _ in range(D1 * D2)]
        for b in range(R):
            rows = last[half, b * D3 : (b + 1) * D3, :]
            for p in range(D1 * D2):
                totals[p] += left[p * R + b : p * R + b + 1, lanes] * rows
        for p in range(D1 * D2):
            out[p * D3 : (p + 1) * D3, lanes] = totals[p]
        return 0

    lax.fori_loop(0, looks // LANES, one, 0)


def expand_grad_left(grad, last, out, lanes):
    turned = [last[pl.ds(d, R, stride=D3), :] for d in range(D3)]
    for p in range(D1 * D2):
        total = jnp.zeros((R, LANES), F32)
        for d in range(D3):
            total += grad[p * D3 + d : p * D3 + d + 1, lanes] * turned[d]
        out[p * R : (p + 1) * R, lanes] = total


def expand_grad_last(left, grad, out, looks):
    def one(half, _):
        lanes = lanes_of(half)
        rows = [grad[p * D3 : (p + 1) * D3, lanes] for p in range(D1 * D2)]
        for b in range(R):
            terms = [left[p * R + b : p * R + b + 1, lanes] * rows[p] for p in range(D1 * D2)]
            while len(terms) > 1:
                terms = [x + y for x, y in zip(terms[::2], terms[1::2])]
            out[b * D3 : (b + 1) * D3, lanes] = terms[0]
        return 0

    lax.fori_loop(0, looks // LANES, one, 0)


def expand_grad_first(grad_left, middle, out, looks):
    group = 8

    def block(half, _):
        lanes = lanes_of(half)
        for base in range(0, R, group):
            totals = [[None] * group for _ in range(D1)]
            for part in range(0, D2 * R, 8):
                rows = [
                    middle[(base + a) * D2 * R + part : (base + a) * D2 * R + part + 8, lanes]
                    for a in range(group)
                ]
                for i in range(D1):
                    weight = grad_left[i * D2 * R + part : i * D2 * R + part + 8, lanes]
                    for a in range(group):
                        term = weight * rows[a]
                        totals[i][a] = totals[i][a] + term if part else term
            for i in range(D1):
                for a in range(group):
                    out[half, pl.ds(i * R + base + a, 8, stride=D1 * R), :] = totals[i][a]
        return 0

    lax.fori_loop(0, looks // LANES, block, 0)


def local_kernel(
    sizes,
    bags,
    one,
    two,
    three,
    labels,
    core_one,
    core_two,
    core_three,
    dense,
    w_top,
    bias,
    w_out,
    keep,
    send,
    shared,
    first,
    middle,
    last,
    left,
    emb,
    grad,
    grad_left,
    grad_last,
    grad_first,
    total,
):
    n1, n2, n3, hid, samples, looks, nx, chunk = sizes
    width = D1 * D2 * D3
    hot_one = one_hot_rows(one[...], n1)
    hot_two = one_hot_rows(two[...], n2)
    hot_three = one_hot_rows(three[...], n3)
    hot_bag = one_hot_rows(bags[...], samples)
    first[...] = dot(core_one[...], hot_one, TN)
    found = dot(core_three[...], hot_three, TN)
    for half in range(looks // LANES):
        last[half] = found[:, half * LANES : (half + 1) * LANES]
    piece = 256
    for c in range(R * D2 * R // piece):
        middle[c * piece : (c + 1) * piece, :] = dot(
            core_two[:, c * piece : (c + 1) * piece], hot_two, TN
        )
    expand_left(first, middle, left, looks)
    expand_embedded(left, last, emb, looks)

    pooled = sum(dot(hot_bag, term, NT) for term in split(emb[...], 3))
    joined = jnp.concatenate([dense[...], pooled.astype(BF16)], axis=1)
    pre = nn(joined, w_top[...]) + bias[...]
    sig = jax.nn.sigmoid(pre)
    hidden = pre * sig
    weight = w_out[...]
    logit = jnp.sum(hidden * weight, axis=1, keepdims=True)
    grid = (samples, samples)
    same = lax.broadcasted_iota(jnp.int32, grid, 0) == lax.broadcasted_iota(jnp.int32, grid, 1)
    wanted = jnp.sum(jnp.where(same, labels[...].astype(F32), 0.0), axis=1, keepdims=True)
    dlogit = (jax.nn.sigmoid(logit) - wanted) / samples
    dpre = dlogit * weight * (sig * (1.0 + pre * (1.0 - sig)))
    low = dpre.astype(BF16)
    w_low = w_top[width : 2 * width, :]
    shared[0:samples, :] = dot(low, w_low, NT)
    for at, row in enumerate((bags, one, two, three)):
        for half in range(looks // LANES):
            spot = samples + at * (looks // LANES) + half
            shared[spot : spot + 1, :] = row[0:1, half * LANES : (half + 1) * LANES].astype(F32)

    turned = dot(w_low, low, NT)
    grad[...] = sum(nn(term, hot_bag) for term in split(turned))

    def back(half, _):
        expand_grad_left(grad, last.at[half], grad_left, lanes_of(half))
        return 0

    lax.fori_loop(0, looks // LANES, back, 0)
    expand_grad_last(left, grad, grad_last, looks)
    expand_grad_first(grad_left, middle, grad_first, looks)

    tops, ones, lasts, _ = sections(n1, n3, hid, 2 * width + 2)
    grad_weight = dot(joined, low, TN)
    grad_bias = jnp.sum(dpre, axis=0, keepdims=True)
    grad_output = jnp.sum(hidden * dlogit, axis=0, keepdims=True)
    total[...] = jnp.zeros(total.shape, F32)
    for half, start in enumerate(tops):
        cut = slice(half * LANES, (half + 1) * LANES)
        total[start : start + 2 * width, :] = grad_weight[:, cut]
        total[start + 2 * width : start + 2 * width + 1, :] = grad_bias[:, cut]
        total[start + 2 * width + 1 : start + 2 * width + 2, :] = grad_output[:, cut]
    wide = jnp.concatenate([grad_first[half] for half in range(looks // LANES)], axis=1)
    found = sum(dot(hot_one, term, NT) for term in split(wide))
    total[ones : ones + n1, :] = tree([found[:, at * LANES : (at + 1) * LANES] for at in range(8)])
    for half, start in enumerate(lasts):
        cut = slice(half * LANES, (half + 1) * LANES)
        total[start : start + n3, :] = sum(
            dot(hot_three, term, NT) for term in split(grad_last[cut, :])
        )

    gx = lax.axis_index("gx")
    for key in range(nx):
        target = keep if key % 2 == 0 else send
        target[key // 2] = total[pl.ds(pl.multiple_of((gx ^ key) * chunk, 8), chunk), :]


def previous(x, amount):
    rows = x.shape[0]
    down, across = divmod(amount, LANES)
    if across:
        x = pltpu.roll(x, LANES - across, axis=1)
        lane = lax.broadcasted_iota(jnp.int32, x.shape, 1)
        x = jnp.where(lane < LANES - across, x, pltpu.roll(x, rows - 1, axis=0))
    if down:
        x = pltpu.roll(x, rows - down, axis=0)
    return x


def spans(index, share, n1, n2):
    length = R * D2 * R
    rows = min((share + 2 * length - 2) // length, n2)
    begin = index * share - n1 * D1 * R
    row = jnp.minimum(lax.div(jnp.maximum(begin, 0), length), n2 - rows)
    return rows, begin, row


def owner_kernel(sizes, index, near, far, core_one, core_three, window, fields, turned, core_first, core_last, last, grad, grad_left):
    n1, n2, n3, share, samples, looks, height, blocks = sizes
    per = looks // LANES
    rows, _, low_row = spans(index[0], share, n1, n2)
    core_first[...] = core_one[...].astype(F32).T.astype(BF16)
    core_last[...] = core_three[...].astype(F32).T.astype(BF16)
    names = []
    for at in range(4):
        pieces = [
            table[k * height + samples + at * per : k * height + samples + (at + 1) * per, :]
            for table in (near, far)
            for k in range(blocks // 2)
        ]
        names.append(jnp.concatenate(pieces, axis=0).astype(jnp.int32))
    bag, one, two, three = names
    total = blocks * per
    line = lax.broadcasted_iota(jnp.int32, (total, LANES), 0)
    flat = line * LANES + lax.broadcasted_iota(jnp.int32, (total, LANES), 1)
    local = two - low_row
    inside = (local >= 0) & (local < rows)
    low_bits, mid_bits, top_bits = ((count - 1).bit_length() for count in (n1, n3, rows))
    mark = 1 << (low_bits + mid_bits + top_bits)
    code = mark | (local << (low_bits + mid_bits)) | (three << low_bits) | one
    code = jnp.where(inside, code, 0)
    sample = bag + lax.div(line, per) * height
    mask = jnp.where(inside, 1.0, 0.0).astype(BF16)
    upper = lax.broadcasted_iota(jnp.int32, (LANES, LANES), 0) < lax.broadcasted_iota(
        jnp.int32, (LANES, LANES), 1
    )
    lower = lax.broadcasted_iota(jnp.int32, (total, total), 1) < lax.broadcasted_iota(
        jnp.int32, (total, total), 0
    )
    within = nn(mask, jnp.where(upper, 1.0, 0.0).astype(BF16))
    above = jnp.sum(nn(jnp.where(lower, 1.0, 0.0).astype(BF16), mask), axis=1, keepdims=True)
    rank = (within + above).astype(jnp.int32)
    count = jnp.sum(mask.astype(F32)).astype(jnp.int32)
    way = jnp.where(inside, flat - rank, 0)
    size = 1
    while size < total * LANES:
        moved, next_code = previous(way, size), previous(code, size)
        take = ((moved & size) != 0) & (flat < total * LANES - size) & (next_code > 0)
        leave = (way & size) != 0
        code = jnp.where(take, next_code, jnp.where(leave, 0, code))
        sample = jnp.where(take, previous(sample, size), sample)
        way = jnp.where(take, moved - size, jnp.where(leave, 0, way))
        size *= 2
    fields[...] = jnp.zeros(fields.shape, F32)
    fields[0, 0:total, :] = code.astype(F32)
    fields[1, 0:total, :] = sample.astype(F32)

    pieces, _, piece = turned.shape

    def flip(c, _):
        spot = pl.ds(pl.multiple_of(c * piece, 8), piece)
        for side, table in enumerate((near, far)):
            for at, term in enumerate(split(table[spot, :].T)):
                turned[side * (pieces // 2) + c, at * LANES : (at + 1) * LANES, :] = term
        return 0

    lax.fori_loop(0, pieces // 2, flip, 0, unroll=pieces <= 8)

    window[...] = jnp.zeros(window.shape, F32)
    group = last.shape[0]

    def find(c, sample_row):
        found = nn(turned[c], one_hot_rows(sample_row - c * piece, piece))
        return found[0:LANES] + found[LANES : 2 * LANES]

    def some(step, _):
        taken = []
        for q in range(group):
            spot = step * group + q
            eight = pl.ds(pl.multiple_of(lax.div(spot, 8) * 8, 8), 8)
            pick = lax.broadcasted_iota(jnp.int32, (8, LANES), 0) == lax.rem(spot, 8)
            taken.append(
                [
                    jnp.sum(jnp.where(pick, fields[at, eight, :], 0.0), axis=0, keepdims=True)
                    for at in range(2)
                ]
            )
        codes, spots = (jnp.concatenate(x, axis=1).astype(jnp.int32) for x in zip(*taken))
        live = codes > 0
        spots = jnp.where(live, spots, -1)
        first_row = codes & ((1 << low_bits) - 1)
        last_row = (codes >> low_bits) & ((1 << mid_bits) - 1)
        here_row = jnp.where(live, (codes & (mark - 1)) >> (low_bits + mid_bits), -1)
        first = nn(core_first[...], one_hot_rows(first_row, n1))
        found = nn(core_last[...], one_hot_rows(last_row, n3))
        for q in range(group):
            last[q] = found[:, q * LANES : (q + 1) * LANES]
        if pieces <= 8:
            grad[...] = tree([find(c, spots) for c in range(pieces)])
        else:
            grad[...] = jnp.zeros(grad.shape, F32)

            def more(c, _):
                grad[...] += find(c, spots)
                return 0

            lax.fori_loop(0, pieces, more, 0)
        for q in range(group):
            expand_grad_left(grad, last.at[q], grad_left, pl.ds(q * LANES, LANES))
        here = [here_row == r for r in range(rows)]
        stacked = []
        for i in range(D1):
            part = first[i * R : (i + 1) * R, :]
            picked = [jnp.where(at_row, part, 0.0) for at_row in here]
            stacked.append(jnp.concatenate(picked, axis=0).astype(BF16))
        terms = [split(grad_left[i * D2 * R : (i + 1) * D2 * R, :]) for i in range(D1)]
        sides = [jnp.concatenate([term[at] for term in terms], axis=1) for at in range(2)]
        found = dot(jnp.concatenate(stacked, axis=1), jnp.concatenate(sides, axis=0), NT)
        window[...] += found[:, 0 : D2 * R] + found[:, D2 * R : 2 * D2 * R]
        return 0

    step_size = group * LANES
    lax.fori_loop(0, lax.div(count + step_size - 1, step_size), some, 0)


def final_kernel(sizes, index, chips, others, window, top, core, total, source):
    n1, n2, n3, hid, _, share, nx, chunk, out_rows = sizes
    width = D1 * D2 * D3
    gx = lax.axis_index("gx")
    for key in range(nx):
        origin = chips if key % 2 == 0 else others
        total[pl.ds(pl.multiple_of((gx ^ key) * chunk, 8), chunk), :] = origin[key // 2]
    rows, begin, row = spans(index[0], share, n1, n2)
    start = n1 * D1 * R + begin - row * R * D2 * R
    top_rows = 2 * width + 2
    tops, ones, lasts, _ = sections(n1, n3, hid, top_rows)
    for half, at in enumerate(tops):
        top[:, half * LANES : (half + 1) * LANES] = total[at : at + top_rows, :]
    source[0:n1, :] = total[ones : ones + n1, :]
    wide = rows * R
    source[n1 : n1 + wide, :] = window[...]
    for half, at in enumerate(lasts):
        source[pl.ds(n1 + wide + half, n3, stride=len(lasts)), :] = total[at : at + n3, :]
    upper = source[pl.ds(lax.div(start, LANES), out_rows), :]
    lower = source[pl.ds(lax.div(start, LANES) + 1, out_rows), :]
    shift = lax.rem(start, LANES)
    turn = (LANES - shift) % LANES
    lane = lax.broadcasted_iota(jnp.int32, upper.shape, 1)
    core[...] = jnp.where(
        lane < LANES - shift, pltpu.roll(upper, turn, axis=1), pltpu.roll(lower, turn, axis=1)
    )


def in_vmem(x):
    small = x.size * x.dtype.itemsize <= 4 * 1024 * 1024
    return pltpu.with_memory_space_constraint(x, pltpu.VMEM) if small else x


def send_xor(x, axis, size, mask):
    return lax.ppermute(x, axis, [(j, j ^ mask) for j in range(size)])


def tree(terms):
    while len(terms) > 1:
        pairs = [x + y for x, y in zip(terms[::2], terms[1::2])]
        terms = pairs + ([terms[-1]] if len(terms) % 2 else [])
    return terms[0]


def per_device(nx, ny, core_one, core_two, core_three, dense_rows, w_top, bias_top, w_out, labels, bag_ids, digit_one, digit_two, digit_three):
    n1, n2, n3 = core_one.shape[0], core_two.shape[0], core_three.shape[0]
    hid = w_top.shape[1]
    samples = dense_rows.shape[0]
    looks = bag_ids.shape[1]
    width = D1 * D2 * D3
    per = looks // LANES
    blocks = nx * ny
    _, _, _, rows_all = sections(n1, n3, hid, 2 * width + 2)
    chunk = up(up(rows_all, nx) // nx, 8)
    height = up(samples + 4 * per, 8)

    vmem = pl.BlockSpec(memory_space=pltpu.VMEM)
    smem = pl.BlockSpec(memory_space=pltpu.SMEM)
    index = (lax.axis_index("gx") * ny + lax.axis_index("gy")).astype(jnp.int32).reshape(1)
    params = pltpu.CompilerParams(vmem_limit_bytes=VMEM_LIMIT)
    sizes = (n1, n2, n3, hid, samples, looks, nx, chunk)
    keep, send, shared = pl.pallas_call(
        functools.partial(local_kernel, sizes),
        out_shape=(
            pltpu.VMEM((nx // 2, chunk, LANES), F32),
            pltpu.VMEM((nx // 2, chunk, LANES), F32),
            pltpu.VMEM((height, LANES), F32),
        ),
        in_specs=[vmem] * 12,
        out_specs=(vmem, vmem, vmem),
        scratch_shapes=[
            pltpu.VMEM((D1 * R, looks), F32),
            pltpu.VMEM((R * D2 * R, looks), F32),
            pltpu.VMEM((looks // LANES, R * D3, LANES), F32),
            pltpu.VMEM((D1 * D2 * R, looks), F32),
            pltpu.VMEM((width, looks), F32),
            pltpu.VMEM((width, looks), F32),
            pltpu.VMEM((D1 * D2 * R, looks), F32),
            pltpu.VMEM((R * D3, looks), F32),
            pltpu.VMEM((looks // LANES, 8 * D1 * R, LANES), F32),
            pltpu.VMEM((nx * chunk, LANES), F32),
        ],
        compiler_params=params,
        cost_estimate=pl.CostEstimate(flops=4_000_000_000, bytes_accessed=4_000_000, transcendentals=0),
        name="local",
    )(
        bag_ids,
        digit_one,
        digit_two,
        digit_three,
        labels.reshape(1, samples),
        core_one,
        core_two,
        core_three,
        dense_rows,
        w_top,
        bias_top.reshape(1, hid),
        w_out.reshape(1, hid),
    )

    half = keep + send_xor(send, "gx", nx, 1)
    tables = [send_xor(shared, "gy", ny, k) for k in range(1, ny)]
    sums = [send_xor(half[k], "gx", nx, 2 * k) for k in range(1, nx // 2)]
    mine = tree([half[0], *sums])
    others = [mine] + [send_xor(mine, "gy", ny, k) for k in range(1, ny)]
    tables, _ = lax.optimization_barrier((tables, others[1:2]))
    table = jnp.concatenate([shared, *tables], axis=0)
    mine = tree(others)
    planes = [send_xor(table, "gx", nx, 2 * k) for k in range(1, nx // 2)]
    chips = [mine] + [send_xor(mine, "gx", nx, 2 * k) for k in range(1, nx // 2)]
    planes, _ = lax.optimization_barrier((planes, chips[1:2]))
    table = jnp.concatenate([table, *planes], axis=0)
    far = send_xor(table, "gx", nx, 1)
    chips = jnp.stack(chips)
    others = send_xor(chips, "gx", nx, 1)
    near, far, chips, others = (in_vmem(x) for x in (table, far, chips, others))

    share = (core_one.size + core_two.size + core_three.size) // blocks
    length = R * D2 * R
    rows = min((share + 2 * length - 2) // length, n2)
    group = up(blocks * looks * rows // n2, LANES) // LANES
    owner = pl.pallas_call(
        functools.partial(owner_kernel, (n1, n2, n3, share, samples, looks, height, blocks)),
        out_shape=pltpu.VMEM((rows * R, LANES), F32),
        in_specs=[smem] + [vmem] * 4,
        out_specs=vmem,
        scratch_shapes=[
            pltpu.VMEM((2, up(blocks * per + group, 8), LANES), F32),
            pltpu.VMEM((blocks // 8, 2 * LANES, 8 * height), BF16),
            pltpu.VMEM((D1 * R, n1), BF16),
            pltpu.VMEM((R * D3, n3), BF16),
            pltpu.VMEM((group, R * D3, LANES), F32),
            pltpu.VMEM((width, group * LANES), F32),
            pltpu.VMEM((D1 * D2 * R, group * LANES), F32),
        ],
        compiler_params=params,
        cost_estimate=pl.CostEstimate(flops=4_000_000_000, bytes_accessed=2_000_000, transcendentals=0),
        name="owner",
    )
    window = owner(index, near, far, core_one, core_three)

    out_rows = up(share, LANES) // LANES
    source_rows = up(n1 + rows * R + n3 * (R * D3 // LANES) + out_rows, 8)
    top, core = pl.pallas_call(
        functools.partial(final_kernel, (n1, n2, n3, hid, ny, share, nx, chunk, out_rows)),
        out_shape=(
            jax.ShapeDtypeStruct((2 * width + 2, hid), F32),
            jax.ShapeDtypeStruct((out_rows, LANES), F32),
        ),
        in_specs=[smem] + [vmem] * 3,
        out_specs=(vmem, vmem),
        scratch_shapes=[
            pltpu.VMEM((nx * chunk, LANES), F32),
            pltpu.VMEM((source_rows, LANES), F32),
        ],
        compiler_params=params,
        name="final",
    )(index, chips, others, in_vmem(window))
    return core.reshape(-1)[:share], top


def solution(mesh):
    both = ("gx", "gy")
    nx, ny = mesh.shape["gx"], mesh.shape["gy"]

    def step(*args):
        return per_device(nx, ny, *args)

    return jax.shard_map(
        step,
        mesh=mesh,
        in_specs=(
            P(),
            P(),
            P(),
            P(both, None),
            P(),
            P(),
            P(),
            P(both),
            P(both, None),
            P(both, None),
            P(both, None),
            P(both, None),
        ),
        out_specs=(P(both), P()),
        check_vma=False,
    )
```
